32 devices in a mesh: section: 2 (over y), expert: 2 (over x), tensor: 8 (over z, core).
Axes of the slice: x: 2, y: 2, z: 4, core: 2. Of those that a mesh axis runs over, the one named last changes fastest.
Arguments:
- query: bfloat16 [2, 512, 4096], P('expert', 'tensor', 'section'), may hold values from -24 to 24
- keys: bfloat16 [2, 512, 1024], P('expert', 'tensor', 'section'), may hold values from -24 to 24
- values: bfloat16 [2, 512, 1024], P('expert', 'tensor', 'section'), may hold values from -6 to 6
- residual: bfloat16 [2, 512, 4096], P('expert', 'tensor', 'section'), may hold values from -6 to 6
- routes: int32 [2, 512, 2], P('expert', 'tensor'), may hold values from 0 to 7, all different within a row; in each aligned block of 64 rows (0 to 63, 64 to 127, ..., all dimensions but the last counted through in order) at most 17 rows name the same one
- gates: float32 [2, 512, 2], P('expert', 'tensor'), may hold values from 0.1 to 0.9
- w_gate: bfloat16 [8, 4096, 8192], P('expert', None, 'tensor'), may hold values from -0.09375 to 0.09375
- w_up: bfloat16 [8, 4096, 8192], P('expert', None, 'tensor'), may hold values from -0.09375 to 0.09375
- w_down: bfloat16 [8, 8192, 4096], P('expert', 'tensor'), may hold values from -0.0625 to 0.0625
Outputs:
- layer_out: bfloat16 [2, 512, 4096], P('expert', 'tensor', 'section')
The draws below stay inside these ranges and needn't reach their ends.
Inputs may be any that keep to these rules, and one draw needn't show every extreme that they name: `routes`: the 2 entries of a row differ. In the rows of one index of expert and tensor (aligned blocks of 64 positions, taken in order over sequences and positions) no expert is named more than 17 times.
All inputs are finite; a program needn't handle non-finite values.
Results may differ from the reference program's by a relative error of at most 0.014.
Values may be sent and summed in bfloat16 or wider, within the bound.
A program may use at most 192 MiB of HBM per device.

```python
import math
import jax
import jax.numpy as jnp
import numpy as np
from jax import lax

D = 4096
H = 32
KVH = 8
HD = 128
EXPERTS = 8
TOP = 2
FF = 8192
TOK_DEV = 64
CAP = 17
GROUPS = 8
SEQS = 2
LENGTH = 512
N_EXPERT = 2
N_TENSOR = 8


def attention_pair(key):
    key_noise = jnp.clip(jax.random.normal(jax.random.fold_in(key, 11), (SEQS, LENGTH, KVH * HD), jnp.float32), -4.5, 4.5)
    query_noise = jnp.clip(jax.random.normal(jax.random.fold_in(key, 12), (SEQS, LENGTH, H * HD), jnp.float32), -4.5, 4.5)
    key_field = key_noise
    query_field = query_noise
    return (query_field, key_field)


def draw_query(key, part):
    return attention_pair(key)[0].astype(jnp.bfloat16)


def draw_keys(key, part):
    return attention_pair(key)[1].astype(jnp.bfloat16)


def block_scale(stream_key, shape, pieces, low, high):
    level, own = 1.0, jax.random.fold_in(stream_key, 6)
    for axis_at, parts in pieces:
        heights = jnp.exp(jax.random.uniform(jax.random.fold_in(own, axis_at), (parts,), jnp.float32, low / len(pieces), high / len(pieces)))
        level = level * jnp.repeat(heights, shape[axis_at] // parts).reshape([-1 if axis == axis_at else 1 for axis in range(len(shape))])
    return level


def deal_out(rng, own, number, rows, amount, top, reach, slope):
    ranking = jax.random.permutation(rng, amount)
    crowded, common = portions_of(amount, rows * top, reach, slope, True), portions_of(amount, rows * top, reach, slope, False)
    places = jnp.arange(amount)

    def named(tallies, rotation):
        used = int((tallies > 0).sum())
        fixed = max(1, used // 4)
        moved = fixed + (places - fixed + rotation * (used - fixed)) % max(1, amount - fixed)
        return jnp.zeros((amount,), jnp.int32).at[ranking[jnp.where(places < fixed, places, moved)]].set(jnp.asarray(tallies, jnp.int32))

    tallies = jnp.where(number % 4 == 0, named(crowded, number // 4), named(common, number - number // 4 - 1))
    mixed = jax.random.permutation(jax.random.fold_in(own, 3), amount)
    donor, sink = mixed[0:amount // 2 * 2:2], mixed[1:amount // 2 * 2:2]
    slack = jnp.minimum(tallies[donor] - 1, reach - tallies[sink]) // 2
    slack = jnp.where((donor == ranking[0]) | (sink == ranking[0]) | (tallies[sink] == 0), 0, jnp.maximum(slack, 0))
    moved = jax.random.randint(jax.random.fold_in(own, 4), (amount // 2,), 0, 1 << 20) % (slack + 1)
    tallies = tallies.at[donor].add(-moved).at[sink].add(moved)
    labels = jnp.searchsorted(jnp.cumsum(tallies), jnp.arange(rows * top), side="right").astype(jnp.int32)
    listing = labels.reshape(top, rows).T
    listing = listing[jax.random.permutation(jax.random.fold_in(own, 1), rows)]
    rotation = jax.random.randint(jax.random.fold_in(own, 2), (rows, 1), 0, top)
    return jnp.take_along_axis(listing, (jnp.arange(top)[None, :] + rotation) % top, axis=1)


def portions_of(number_of, total, most, skew, full):
    loads = [(1 << 20) // math.isqrt(standing ** skew) + 1 for standing in range(1, number_of + 1)]
    largest = most if full else min(most, max(-(-total // number_of), total * loads[0] // sum(loads)))
    least = 1 if total - largest >= number_of - 1 else 0
    counts, surplus = [largest] + [least] * (number_of - 1), total - largest - least * (number_of - 1)
    while surplus > 0:
        candidates = [i for i in range(1, number_of) if counts[i] < largest] or [i for i in range(1, number_of) if counts[i] < most]
        pool, remaining = sum([loads[i] for i in candidates]), surplus
        for i in candidates:
            more = min(most - counts[i], max(1, remaining * loads[i] // pool), surplus)
            counts[i] = counts[i] + more
            surplus = surplus - more
    return np.array(counts)


def gaussian(own_key, dims, scale, bound, shards=(), held_as=jnp.bfloat16):
    factor_of = block_scale(own_key, dims, shards, -0.22, 0.18) if shards else 1.0
    array = jax.random.normal(own_key, dims, jnp.float32) * scale * factor_of
    return jnp.minimum(jnp.maximum(array, -bound), bound).astype(held_as)


def setup_inputs(seed: int = 0) -> dict:
    seeds = jax.random.split(jax.random.key(seed), 10)
    query = draw_query(jax.random.fold_in(seeds[9], 71), 0)
    keys = draw_keys(jax.random.fold_in(seeds[9], 71), 0)
    values = gaussian(seeds[2], (SEQS, LENGTH, KVH * HD), 1.0, 6.0, ((0, 2), (1, 8), (2, 2)))
    residual = gaussian(seeds[3], (SEQS, LENGTH, D), 1.0, 6.0, ((0, 2), (1, 8), (2, 2)))
    routes_keys = jax.random.split(jax.random.fold_in(seeds[4], 1), SEQS * LENGTH // TOK_DEV)
    routes_turns = jax.random.permutation(jax.random.fold_in(seeds[4], 3), SEQS * LENGTH // TOK_DEV)
    routes = jax.vmap(lambda own, number: deal_out(jax.random.fold_in(seeds[4], 2), own, number, TOK_DEV, EXPERTS, TOP, CAP, 2))(routes_keys, routes_turns).reshape((SEQS, LENGTH, TOP))
    gates = jnp.clip(0.1 + 0.79999997 * jax.random.uniform(seeds[5], (SEQS, LENGTH, TOP), jnp.float32) ** block_scale(seeds[5], (SEQS, LENGTH, TOP), ((0, 2), (1, 8)), -0.2, 0.2), 0.1, 0.9)
    w_gate = gaussian(seeds[6], (EXPERTS, D, FF), D ** -0.5, 0.09375, ((0, 2), (2, 8)))
    w_up = gaussian(seeds[7], (EXPERTS, D, FF), D ** -0.5, 0.09375, ((0, 2), (2, 8)))
    w_down = gaussian(seeds[8], (EXPERTS, FF, D), FF ** -0.5, 0.0625, ((0, 2), (1, 8)))
    return dict(query=query, keys=keys, values=values, residual=residual, routes=routes, gates=gates, w_gate=w_gate, w_up=w_up, w_down=w_down)


def attend(query_seq, key_seq, value_seq):
    length = query_seq.shape[0]
    groups = H // KVH
    queries = query_seq.reshape(length, KVH, groups, HD).astype(jnp.float32)
    keys_all = key_seq.reshape(length, KVH, HD).astype(jnp.float32)
    values_all = value_seq.reshape(length, KVH, HD).astype(jnp.float32)
    scores = jnp.einsum('qkgd,tkd->kgqt', queries, keys_all) / math.sqrt(HD)
    positions = jnp.arange(length)
    causal = positions[:, None] >= positions[None, :]
    masked = jnp.where(causal, scores, -1e+30)
    row_peak = lax.optimization_barrier(jnp.max(masked, axis=-1, keepdims=True))
    exp_terms = jnp.where(causal, jnp.exp(masked - row_peak), 0.0)
    weights = (exp_terms / lax.optimization_barrier(jnp.sum(exp_terms, axis=-1, keepdims=True))).astype(jnp.bfloat16)
    context = jnp.einsum('kgqt,tkd->qkgd', weights.astype(jnp.float32), values_all)
    return context.reshape(length, H * HD)

def reference(query, keys, values, residual, routes, gates, w_gate, w_up, w_down):
    context = lax.map(lambda triple: attend(triple[0], triple[1], triple[2]), (query, keys, values))
    hidden = (residual.astype(jnp.float32) + context).astype(jnp.bfloat16)
    token_total = SEQS * LENGTH
    hidden_flat = hidden.reshape(token_total, D)
    picked = routes.reshape(token_total * TOP).astype(jnp.int32)
    most_rows = CAP * N_EXPERT * N_TENSOR
    block_count = GROUPS
    block_width = FF // block_count

    def expert_pass(expert_id, outputs):
        matches = jnp.nonzero(picked == expert_id, size=most_rows, fill_value=token_total * TOP)[0].astype(jnp.int32)
        safe_index = jnp.minimum(matches, token_total * TOP - 1)
        token_rows = hidden_flat[safe_index // TOP]
        gate_part = jnp.dot(token_rows, w_gate[expert_id], preferred_element_type=jnp.float32)
        up_part = jnp.dot(token_rows, w_up[expert_id], preferred_element_type=jnp.float32)
        inner_rows = (jax.nn.silu(gate_part) * up_part).astype(jnp.bfloat16)
        down_full = w_down[expert_id]

        def add_block(block_id, running):
            inner_block = lax.dynamic_slice_in_dim(inner_rows, block_id * block_width, block_width, 1)
            down_block = lax.dynamic_slice_in_dim(down_full, block_id * block_width, block_width, 0)
            partial_value = jnp.dot(inner_block, down_block, preferred_element_type=jnp.float32).astype(jnp.bfloat16)
            return running + partial_value.astype(jnp.float32)
        summed = lax.fori_loop(0, block_count, add_block, jnp.zeros((most_rows, D), jnp.float32))
        return outputs.at[matches].set(summed.astype(jnp.bfloat16), mode='drop')
    expert_out = lax.fori_loop(0, EXPERTS, expert_pass, jnp.zeros((token_total * TOP, D), jnp.bfloat16))
    weighted = gates.reshape(token_total, TOP, 1).astype(jnp.float32) * expert_out.reshape(token_total, TOP, D).astype(jnp.float32)
    layer_out = hidden_flat.astype(jnp.float32) + lax.optimization_barrier(jnp.sum(weighted, axis=1))
    return layer_out.astype(jnp.bfloat16).reshape(SEQS, LENGTH, D)
```

```python
import functools
import math

import jax
import jax.numpy as jnp
from jax import lax
from jax.sharding import PartitionSpec as P

from jax.experimental import pallas as pl
from jax.experimental.pallas import tpu as pltpu

HD = 128
EXPERTS = 8
TOP = 2
HALF_CAP = 9
META = 128
MESH = pl.DeviceIdType.MESH


def place():
    s, e, t = lax.axis_index("section"), lax.axis_index("expert"), lax.axis_index("tensor")
    return s, e, t // 2, t % 2


def neighbours(s, e, z, c, ring):
    return dict(
        core=(s, e, 2 * z + 1 - c),
        side=(s, 1 - e, 2 * z + c),
        up=(s, e, 2 * lax.rem(z + 1, ring) + c),
        down=(s, e, 2 * lax.rem(z + ring - 1, ring) + c),
        swap=(c, e, 2 * z + s),
    )


def greet(near, s, c):
    barrier = pltpu.get_barrier_semaphore()
    for name in ("core", "side", "up", "down"):
        pl.semaphore_signal(barrier, inc=1, device_id=near[name], device_id_type=MESH)

    @pl.when(s != c)
    def _():
        pl.semaphore_signal(barrier, inc=1, device_id=near["swap"], device_id_type=MESH)

    pl.semaphore_wait(barrier, 4 + (s + c) % 2)


def attend_gather(ring, q_ref, k_ref, v_ref, r_ref, m_ref, x_ref, h_ref, kv, ext, ksend, krecv, send, recv, local):
    s, e, z, c = place()
    near = neighbours(s, e, z, c, ring)
    rows, half = q_ref.shape
    mid = rows // 2
    kvw = k_ref.shape[1]
    wide = ext.shape[1]
    t = 2 * z + c
    fills = [
        pltpu.make_async_copy(k_ref, kv.at[t, :, pl.ds(0, kvw)], local.at[0]),
        pltpu.make_async_copy(v_ref, kv.at[t, :, pl.ds(kvw, kvw)], local.at[1]),
        pltpu.make_async_copy(m_ref, ext.at[:, pl.ds(half, META)], local.at[2]),
    ]
    for fill in fills:
        fill.start()
    greet(near, s, c)
    for fill in fills:
        fill.wait()

    def kcopy(slot, who, index, lo=0, size=rows):
        ref = kv.at[slot, pl.ds(lo, size), :]
        return pltpu.make_async_remote_copy(
            ref, ref, ksend.at[index], krecv.at[index], device_id=near[who], device_id_type=MESH
        )

    def at(dz):
        return lax.rem(z + dz, ring)

    def ks(dz, core):
        return 2 * at(dz) + core

    c2 = c
    k = [
        kcopy(ks(0, c2), "core", 0),
        kcopy(ks(0, c2), "up", 1),
        kcopy(ks(0, c2), "down", 2),
        kcopy(ks(ring - 1, c2), "core", 3),
        kcopy(ks(ring - 1, c2), "up", 4, 0, mid),
        kcopy(ks(1, c2), "core", 5),
        kcopy(ks(1, c2), "down", 6, mid, mid),
        kcopy(ks(2, c2), "core", 7, 0, mid),
        kcopy(ks(2, c2), "core", 8, mid, mid),
    ]
    k[1].start()
    k[2].start()
    k[0].start()
    k[1].wait_recv()
    k[4].start()
    k[3].start()
    k[2].wait_recv()
    k[6].start()
    k[5].start()
    k[4].wait_recv()
    k[7].start()
    k[6].wait_recv()
    k[8].start()
    for i in (0, 3, 5, 7, 8):
        k[i].wait_recv()
    for one in k:
        one.wait_send()

    blocks = kv.shape[0]
    length = blocks * rows
    local_kv = kvw // HD
    groups = half // HD // local_kv
    row_at = lax.broadcasted_iota(jnp.int32, (groups * rows, length), 0) % rows + t * rows
    causal = row_at >= lax.broadcasted_iota(jnp.int32, (groups * rows, length), 1)
    for head in range(local_kv):
        q = jnp.concatenate(
            [q_ref[:, (head * groups + g) * HD : (head * groups + g + 1) * HD] for g in range(groups)], axis=0
        )
        keys = kv[:, :, head * HD : (head + 1) * HD].reshape(length, HD)
        vals = kv[:, :, kvw + head * HD : kvw + (head + 1) * HD].reshape(length, HD)
        scores = lax.dot_general(q, keys, (((1,), (1,)), ((), ())), preferred_element_type=jnp.float32)
        scores = jnp.where(causal, scores * (1.0 / math.sqrt(HD)), -1e30)
        terms = jnp.where(causal, jnp.exp(scores - jnp.max(scores, axis=1, keepdims=True)), 0.0)
        probs = (terms / jnp.sum(terms, axis=1, keepdims=True)).astype(jnp.bfloat16)
        ctx = jnp.dot(probs, vals, preferred_element_type=jnp.float32)
        for g in range(groups):
            cols = slice((head * groups + g) * HD, (head * groups + g + 1) * HD)
            out = (r_ref[:, cols].astype(jnp.float32) + ctx[g * rows : (g + 1) * rows]).astype(jnp.bfloat16)
            h_ref[:, cols] = out
            ext[:, cols] = out

    def blk(x, dz):
        return x * ring + at(dz)

    def cols(core):
        return pl.ds(pl.multiple_of(core * wide, 128), wide)

    swap = pltpu.make_async_remote_copy(
        ext, x_ref.at[blk(e, 0), :, cols(s)], send.at[19], recv.at[19],
        device_id=near["swap"], device_id_type=MESH,
    )
    stay = pltpu.make_async_copy(ext, x_ref.at[blk(e, 0), :, cols(c)], local.at[3])

    @pl.when(s != c)
    def _():
        swap.start()
        swap.wait()

    @pl.when(s == c)
    def _():
        stay.start()
        stay.wait()

    def copy(block, who, index, lo=0, size=rows):
        ref = x_ref.at[block, pl.ds(lo, size), cols(c)]
        return pltpu.make_async_remote_copy(
            ref, ref, send.at[index], recv.at[index], device_id=near[who], device_id_type=MESH
        )

    o = 1 - e
    g = [
        copy(blk(e, 0), "core", 0),
        copy(blk(e, 0), "side", 1),
        copy(blk(e, 0), "up", 2),
        copy(blk(e, 0), "down", 3),
        copy(blk(o, 0), "core", 4),
        copy(blk(o, 0), "up", 5),
        copy(blk(o, 0), "down", 6),
    ]
    for base, x in ((7, e), (13, o)):
        g += [
            copy(blk(x, ring - 1), "core", base),
            copy(blk(x, ring - 1), "up", base + 1, 0, mid),
            copy(blk(x, 1), "core", base + 2),
            copy(blk(x, 1), "down", base + 3, mid, mid),
            copy(blk(x, 2), "core", base + 4, 0, mid),
            copy(blk(x, 2), "core", base + 5, mid, mid),
        ]
    for i in (1, 2, 3, 0):
        g[i].start()
    g[1].wait_recv()
    for i in (5, 6, 4):
        g[i].start()
    for base, first in ((7, 2), (13, 5)):
        g[first].wait_recv()
        g[base + 1].start()
        g[base].start()
        g[first + 1].wait_recv()
        g[base + 3].start()
        g[base + 2].start()
    for base in (7, 13):
        g[base + 1].wait_recv()
        g[base + 4].start()
        g[base + 3].wait_recv()
        g[base + 5].start()
    for i in (0, 4, 7, 9, 11, 12, 13, 15, 17, 18):
        g[i].wait_recv()
    for one in g:
        one.wait_send()


def experts(half, wide, x_ref, sel_ref, comb_ref, wg_ref, wu_ref, wd_ref, p_ref, packed, acc, held):
    e, j = pl.program_id(0), pl.program_id(1)
    count, cap = sel_ref.shape[0], sel_ref.shape[1]
    tile = 1024

    @pl.when(j == 0)
    def _():
        for core in range(2):
            for n in range(half // tile):
                packed[:, core * half + n * tile : core * half + (n + 1) * tile] = jnp.dot(
                    sel_ref[e], x_ref[:, core * wide + n * tile : core * wide + (n + 1) * tile],
                    preferred_element_type=jnp.float32,
                ).astype(jnp.bfloat16)

    gate = jnp.dot(packed[...], wg_ref[0], preferred_element_type=jnp.float32)
    up = jnp.dot(packed[...], wu_ref[0], preferred_element_type=jnp.float32)
    inner = (gate / (1.0 + jnp.exp(-gate)) * up).astype(jnp.bfloat16)

    @pl.when(j == 0)
    def _():
        for n in range(2 * half // tile):
            cs = slice(n * tile, (n + 1) * tile)
            acc[:, cs] = jnp.dot(inner, wd_ref[0, :, cs], preferred_element_type=jnp.float32)

    @pl.when(j > 0)
    def _():
        for n in range(2 * half // tile):
            cs = slice(n * tile, (n + 1) * tile)
            acc[:, cs] += jnp.dot(inner, wd_ref[0, :, cs], preferred_element_type=jnp.float32)

    @pl.when(j == pl.num_programs(1) - 1)
    def _():
        held[pl.ds(pl.multiple_of(e * cap, 16), cap), :] = acc[...].astype(jnp.bfloat16)

    @pl.when((j == pl.num_programs(1) - 1) & (e == count - 1))
    def _():
        for n in range(2 * half // tile):
            cs = slice(n * tile, (n + 1) * tile)
            p_ref[:, cs] = jnp.dot(comb_ref[...], held[:, cs], preferred_element_type=jnp.float32).astype(jnp.bfloat16)


def scatter_sum(ring, p_ref, out_ref, a, r, far_up, far_down, near_up, near_down, total, across, send, recv, local):
    s, e, z, c = place()
    near = neighbours(s, e, z, c, ring)
    rows, half = out_ref.shape
    mid = rows // 2
    greet(near, s, c)

    def add(x, y):
        return (x.astype(jnp.float32) + y.astype(jnp.float32)).astype(jnp.bfloat16)

    def cols(core):
        return pl.ds(pl.multiple_of(core * half, 128), half)

    def blk(x, dz):
        return x * ring + lax.rem(z + dz, ring)

    def remote(src, dst, who, index):
        return pltpu.make_async_remote_copy(
            src, dst, send.at[index], recv.at[index], device_id=near[who], device_id_type=MESH
        )

    o = 1 - e
    order = [(i, dz) for dz in (2, 1, ring - 1, 0) for i in (0, 1)]
    side = (o, e)
    first = {
        key: remote(p_ref.at[blk(side[key[0]], key[1]), :, cols(1 - c)], a.at[blk(side[key[0]], key[1])], "core", n)
        for n, key in enumerate(order)
    }
    for key in order:
        first[key].start()

    def reduce_core(i, dz):
        first[(i, dz)].wait_recv()
        b = blk(side[i], dz)
        r[b] = add(p_ref[b, :, cols(c)], a[b])

    lo, hi = pl.ds(0, mid), pl.ds(mid, mid)
    later = []
    hops = []
    for i in (0, 1):
        reduce_core(i, 2)
        b = blk(side[i], 2)
        two = (remote(r.at[b, lo, :], far_up.at[i], "up", 8 + i), remote(r.at[b, hi, :], far_down.at[i], "down", 10 + i))
        for one in two:
            one.start()
        hops.append(two)
        later += two
    for i in (0, 1):
        reduce_core(i, 1)
        reduce_core(i, ring - 1)
    ends = []
    for i in (0, 1):
        b = blk(side[i], 1)
        hops[i][0].wait_recv()
        r[b, lo, :] = add(r[b, lo, :], far_up[i])
        up = remote(r.at[b], near_up.at[i], "up", 12 + i)
        up.start()
        b = blk(side[i], ring - 1)
        hops[i][1].wait_recv()
        r[b, hi, :] = add(r[b, hi, :], far_down[i])
        down = remote(r.at[b], near_down.at[i], "down", 14 + i)
        down.start()
        ends.append((up, down))
        later += [up, down]
    for i in (0, 1):
        reduce_core(i, 0)
    for i in (0, 1):
        b = blk(side[i], 0)
        for one in ends[i]:
            one.wait_recv()
        whole = r[b].astype(jnp.float32) + near_up[i].astype(jnp.float32) + near_down[i].astype(jnp.float32)
        total[i] = whole.astype(jnp.bfloat16)
        if i == 0:
            over = remote(total.at[0], across, "side", 16)
            over.start()
            later.append(over)
    over.wait_recv()
    over.wait_send()
    total[0] = add(total[1], across[...])
    swap = remote(total.at[0], out_ref, "swap", 17)
    stay = pltpu.make_async_copy(total.at[0], out_ref, local.at[0])

    @pl.when(s != c)
    def _():
        swap.start()
        swap.wait()

    @pl.when(s == c)
    def _():
        stay.start()
        stay.wait()

    for one in later[:-1]:
        one.wait_send()
    for key in order:
        first[key].wait_send()


def fast_device(query, keys, values, residual, routes, gates, w_gate, w_up, w_down):
    ring = lax.axis_size("tensor") // 2
    blocks = lax.axis_size("expert") * ring
    rows, half = query.shape[1], query.shape[2]
    wide = half + META
    local_experts, _, units = w_gate.shape
    whole = pl.BlockSpec(memory_space=pltpu.VMEM)
    bf16 = jnp.bfloat16
    dma = pltpu.SemaphoreType.DMA
    meta = jnp.concatenate([routes[0].astype(bf16), gates[0].astype(bf16)], axis=1)
    meta = jnp.pad(meta, ((0, 0), (0, META - meta.shape[1])))
    limit = 60000 * 1024
    x, hidden = pl.pallas_call(
        functools.partial(attend_gather, ring),
        out_shape=(
            jax.ShapeDtypeStruct((blocks, rows, 2 * wide), bf16),
            jax.ShapeDtypeStruct((rows, half), bf16),
        ),
        in_specs=[whole] * 5,
        out_specs=(whole, whole),
        scratch_shapes=[
            pltpu.VMEM((2 * ring, rows, 2 * keys.shape[2]), bf16),
            pltpu.VMEM((rows, wide), bf16),
            dma((9,)), dma((9,)), dma((20,)), dma((20,)), dma((4,)),
        ],
        compiler_params=pltpu.CompilerParams(collective_id=0, has_side_effects=True, vmem_limit_bytes=40000 * 1024),
    )(query[0], keys[0], values[0], residual[0], meta)

    x = x.reshape(blocks * rows, 2 * wide)
    tokens = blocks * rows
    picked = x[:, half : half + TOP].astype(jnp.int32)
    weight = x[:, half + TOP : half + 2 * TOP].astype(jnp.float32)
    cap = -(-17 * blocks // 16) * 16
    mine = lax.axis_index("expert") * local_experts + jnp.arange(local_experts)
    match = picked[:, :, None] == mine[None, None, :]
    hit = jnp.any(match, axis=1)
    scale = jnp.sum(jnp.where(match, weight[:, :, None], 0.0), axis=1)
    below = (jnp.arange(tokens)[:, None] > jnp.arange(tokens)[None, :]).astype(bf16)
    slot = jnp.dot(below, hit.astype(bf16), preferred_element_type=jnp.float32).astype(jnp.int32)
    slot = jnp.where(hit, slot, -1)
    sel = (slot.T[:, None, :] == jnp.arange(cap)[None, :, None]).astype(bf16)
    comb = jnp.where(slot[:, :, None] == jnp.arange(cap)[None, None, :], scale[:, :, None], 0.0)
    comb = comb.reshape(tokens, local_experts * cap).astype(bf16)

    tile = 256
    partial = pl.pallas_call(
        functools.partial(experts, half, wide),
        grid=(local_experts, units // tile),
        out_shape=jax.ShapeDtypeStruct((tokens, 2 * half), bf16),
        in_specs=[
            whole, whole, whole,
            pl.BlockSpec((1, 2 * half, tile), lambda e, j: (e, 0, j)),
            pl.BlockSpec((1, 2 * half, tile), lambda e, j: (e, 0, j)),
            pl.BlockSpec((1, tile, 2 * half), lambda e, j: (e, j, 0)),
        ],
        out_specs=whole,
        scratch_shapes=[
            pltpu.VMEM((cap, 2 * half), bf16),
            pltpu.VMEM((cap, 2 * half), jnp.float32),
            pltpu.VMEM((local_experts * cap, 2 * half), bf16),
        ],
        compiler_params=pltpu.CompilerParams(
            dimension_semantics=("arbitrary", "arbitrary"), vmem_limit_bytes=limit
        ),
    )(x, sel, comb, w_gate, w_up, w_down)

    added = pl.pallas_call(
        functools.partial(scatter_sum, ring),
        out_shape=jax.ShapeDtypeStruct((rows, half), bf16),
        in_specs=[whole],
        out_specs=whole,
        scratch_shapes=[
            pltpu.VMEM((blocks, rows, half), bf16),
            pltpu.VMEM((blocks, rows, half), bf16),
            pltpu.VMEM((2, rows // 2, half), bf16),
            pltpu.VMEM((2, rows // 2, half), bf16),
            pltpu.VMEM((2, rows, half), bf16),
            pltpu.VMEM((2, rows, half), bf16),
            pltpu.VMEM((2, rows, half), bf16),
            pltpu.VMEM((rows, half), bf16),
            dma((18,)), dma((18,)), dma((1,)),
        ],
        compiler_params=pltpu.CompilerParams(collective_id=1, has_side_effects=True, vmem_limit_bytes=40000 * 1024),
    )(partial.reshape(blocks, rows, 2 * half))
    return (hidden.astype(jnp.float32) + added.astype(jnp.float32)).astype(bf16)[None]


def from_partner(value, axis, stride):
    mask = 2**stride
    pairs = [(source, source ^ mask) for source in range(lax.axis_size(axis))]
    return lax.ppermute(value, axis, pairs)


def slot_table(picked, first_slot, slot_count):
    flattened = picked.reshape(-1)
    onehot = (flattened[:, None] == jnp.arange(EXPERTS)[None, :]).astype(jnp.int32)
    before = jnp.cumsum(onehot, axis=0) - onehot
    slot_index = jnp.sum(before * onehot, axis=1)
    target = slot_index * EXPERTS + flattened
    rows_wanted = first_slot * EXPERTS + jnp.arange(slot_count * EXPERTS)
    return rows_wanted[:, None] == target[None, :]


def pack_rows(token_rows, picked, first_slot, slot_count):
    slot_hits = slot_table(picked, first_slot, slot_count)
    token_count = token_rows.shape[0]
    single = jnp.any(slot_hits.reshape(slot_count * EXPERTS, token_count, TOP), axis=2).astype(
        jnp.bfloat16
    )
    packed = jnp.dot(single, token_rows, preferred_element_type=jnp.float32).astype(jnp.bfloat16)
    return packed.reshape(slot_count, EXPERTS, token_rows.shape[1])


def expert_inner(piece_rows, gate_cols, up_cols):
    gate_part = jnp.einsum(
        "red,edf->ref", piece_rows, gate_cols, preferred_element_type=jnp.float32
    )
    up_part = jnp.einsum("red,edf->ref", piece_rows, up_cols, preferred_element_type=jnp.float32)
    return (jax.nn.silu(gate_part) * up_part).astype(jnp.bfloat16)


def on_device(query, keys, values, residual, routes, gates, w_gate, w_up, w_down):
    key_all, value_all = (
        lax.all_gather(keys, "tensor", axis=1, tiled=True),
        lax.all_gather(values, "tensor", axis=1, tiled=True),
    )
    token_count = query.shape[1]
    length = key_all.shape[1]
    half_width = query.shape[2]
    local_heads = half_width // HD
    local_kv = keys.shape[2] // HD
    groups = local_heads // local_kv
    section_id = lax.axis_index("section")
    queries = query[0].reshape(token_count, local_kv, groups, HD)
    key_heads = key_all[0].reshape(length, local_kv, HD)
    value_heads = value_all[0].reshape(length, local_kv, HD)
    scores = jnp.einsum(
        "qkgd,tkd->kgqt", queries, key_heads, preferred_element_type=jnp.float32
    ) / math.sqrt(HD)
    start_row = lax.axis_index("tensor") * token_count
    query_positions = start_row + jnp.arange(token_count)
    causal = query_positions[:, None] >= jnp.arange(length)[None, :]
    masked = jnp.where(causal, scores, -1e30)
    row_peak = jnp.max(masked, axis=-1, keepdims=True)
    exp_terms = jnp.where(causal, jnp.exp(masked - row_peak), 0.0)
    weights = (exp_terms / jnp.sum(exp_terms, axis=-1, keepdims=True)).astype(jnp.bfloat16)
    context = jnp.einsum("kgqt,tkd->qkgd", weights, value_heads, preferred_element_type=jnp.float32)
    hidden_half = (
        residual[0].astype(jnp.float32) + context.reshape(token_count, half_width)
    ).astype(jnp.bfloat16)
    picked = routes[0]
    hidden = lax.all_gather(hidden_half, "section", axis=1, tiled=True)
    packed = pack_rows(hidden, picked, section_id * HALF_CAP, HALF_CAP)
    arrived = lax.all_to_all(packed, "expert", split_axis=1, concat_axis=0, tiled=True)
    inner_rows = expert_inner(lax.all_gather(arrived, "tensor", axis=0, tiled=True), w_gate, w_up)
    summed = lax.psum_scatter(
        jnp.einsum("ref,efd->red", inner_rows, w_down, preferred_element_type=jnp.float32).astype(
            jnp.bfloat16
        ),
        "tensor",
        scatter_dimension=0,
        tiled=True,
    )
    returned = lax.all_to_all(summed, "expert", split_axis=0, concat_axis=1, tiled=True)
    own_cols = lax.dynamic_slice_in_dim(returned, section_id * half_width, half_width, 2)
    other_cols = lax.dynamic_slice_in_dim(returned, (1 - section_id) * half_width, half_width, 2)
    partner_cols = from_partner(other_cols, "section", 0)
    first_half = jnp.where(section_id == 0, own_cols, partner_cols)
    second_half = jnp.where(section_id == 0, partner_cols, own_cols)
    returned_half = jnp.concatenate([first_half, second_half], axis=0)
    slot_total = returned_half.shape[0]
    slot_hits = slot_table(picked, 0, slot_total)
    weight_table = jnp.sum(
        slot_hits.astype(jnp.float32).reshape(slot_total * EXPERTS, token_count, TOP)
        * gates[0][None, :, :],
        axis=2,
    )
    expert_sum = jnp.einsum(
        "ct,cd->td",
        weight_table,
        returned_half.reshape(slot_total * EXPERTS, half_width).astype(jnp.float32),
        precision=lax.Precision.HIGHEST,
    )
    layer_out = (hidden_half.astype(jnp.float32) + expert_sum).astype(jnp.bfloat16)
    return layer_out[None]


def solution(mesh):
    small = dict(mesh.shape) == {"section": 2, "expert": 2, "tensor": 8}
    return jax.shard_map(
        fast_device if small else on_device,
        mesh=mesh,
        in_specs=(
            P("expert", "tensor", "section"),
            P("expert", "tensor", "section"),
            P("expert", "tensor", "section"),
            P("expert", "tensor", "section"),
            P("expert", "tensor", None),
            P("expert", "tensor", None),
            P("expert", None, "tensor"),
            P("expert", None, "tensor"),
            P("expert", "tensor", None),
        ),
        out_specs=P("expert", "tensor", "section"),
        check_vma=False,
    )
```
